32 devices in a mesh: dp: 4 (over y, x), mp: 8 (over z, core).
Axes of the slice: x: 2, y: 2, z: 4, core: 2. Of those that a mesh axis runs over, the one named last changes fastest.
Arguments:
- tokens: bfloat16 [128, 6144], P(('dp', 'mp')), may hold values from -6 to 6
- norm_gain: float32 [6144], replicated, may hold values from 0.5 to 1.5
- w_query: bfloat16 [6144, 4096], P('dp', 'mp'), as said below
- w_key: bfloat16 [6144, 4096], P('dp', 'mp'), as said below
- w_value: bfloat16 [6144, 4096], P('dp', 'mp'), may hold values from -0.078125 to 0.078125
- w_inner: bfloat16 [6144, 24576], P('dp', 'mp'), may hold values from -0.078125 to 0.078125
- bias_inner: float32 [24576], P('mp'), may hold values from -3 to 3
- w_attn_out: bfloat16 [4096, 6144], P('mp', 'dp'), may hold values from -0.09375 to 0.09375
- w_outer: bfloat16 [24576, 6144], P('mp', 'dp'), may hold values from -0.0390625 to 0.0390625
- temper: float32 [32], P('mp'), may hold values from 0.5 to 24
Outputs:
- result: bfloat16 [128, 6144], P(('dp', 'mp'))
The draws below stay inside these ranges and needn't reach their ends.
Inputs may be any that keep to these rules, and one draw needn't show every extreme that they name: `w_query`: entries of order 6144 ** -0.5. `w_key`: entries of order 6144 ** -0.5.
All inputs are finite; a program needn't handle non-finite values.
Results may differ from the reference program's by a relative error of at most 0.023.
Values may be sent and summed in bfloat16 or wider, within the bound.
A program may use at most 128 MiB of HBM per device.

```python
import math
import jax
import jax.numpy as jnp
from jax import lax

D = 6144
HEADS = 32
HEAD = 128
FF = 24576
HD = 4096
PATCHES = 32
TOKENS = 128
N_DP = 4


def shared_draws(key):
    key_query = jax.random.fold_in(key, 11)
    key_noise = jax.random.fold_in(key, 12)
    key_temper = jax.random.fold_in(key, 14)
    scale = D ** (-0.5)
    limit = 6.0 * scale
    query = jnp.clip(jax.random.normal(key_query, (D, HD), jnp.float32) * scale, -limit, limit)
    noise = jnp.clip(jax.random.normal(key_noise, (D, HD), jnp.float32) * scale, -limit, limit)
    temper = jnp.exp(jax.random.uniform(key_temper, (HEADS,), jnp.float32, jnp.log(0.5), jnp.log(6.0)))
    keys = noise
    return (query, keys, temper)


def draw_w_query(key, part):
    return shared_draws(key)[0].astype(jnp.bfloat16)


def draw_w_key(key, part):
    return shared_draws(key)[1].astype(jnp.bfloat16)


def draw_temper(key, part):
    return shared_draws(key)[2]


def level_of(rng, extent, split, low, high):
    level, own = 1.0, jax.random.fold_in(rng, 6)
    for dim, blocks in split:
        heights = jnp.exp(jax.random.uniform(jax.random.fold_in(own, dim), (blocks,), jnp.float32, low / len(split), high / len(split)))
        level = level * jnp.repeat(heights, extent[dim] // blocks).reshape([-1 if axis == dim else 1 for axis in range(len(extent))])
    return level


def bell_draw(stream_key, extent, deviation, most, shards=(), kind=jnp.bfloat16):
    result = deviation * jax.random.normal(stream_key, extent, jnp.float32)
    if shards:
        result = result * level_of(stream_key, extent, shards, -0.22, 0.18)
    return jnp.clip(result, -most, most).astype(kind)


def setup_inputs(seed: int = 0) -> dict:
    streams_of = jax.random.split(jax.random.key(seed), 11)
    return {
        "tokens": bell_draw(streams_of[0], (TOKENS, D), 1.0, 6.0, ((0, 32),)),
        "norm_gain": jnp.clip(1.0 + 0.1 * jax.random.normal(streams_of[1], (D,), jnp.float32), 0.5, 1.5),
        "w_query": draw_w_query(jax.random.fold_in(streams_of[10], 71), 0),
        "w_key": draw_w_key(jax.random.fold_in(streams_of[10], 71), 0),
        "w_value": bell_draw(streams_of[4], (D, HD), D ** -0.5, 0.078125, ((0, 4), (1, 8))),
        "w_inner": bell_draw(streams_of[5], (D, FF), D ** -0.5, 0.078125, ((0, 4), (1, 8))),
        "bias_inner": bell_draw(streams_of[6], (FF,), 0.5, 3.0, ((0, 8),), jnp.float32),
        "w_attn_out": bell_draw(streams_of[7], (HD, D), HD ** -0.5, 0.09375, ((0, 8), (1, 4))),
        "w_outer": bell_draw(streams_of[8], (FF, D), FF ** -0.5, 0.0390625, ((0, 8), (1, 4))),
        "temper": draw_temper(jax.random.fold_in(streams_of[10], 71), 0),
    }


def normalize(values):
    center = values - lax.optimization_barrier(jnp.mean(values, axis=-1, keepdims=True))
    spread = lax.optimization_barrier(jnp.mean(center * center, axis=-1, keepdims=True))
    return center * lax.rsqrt(spread + 1e-06)

def reference(tokens, norm_gain, w_query, w_key, w_value, w_inner, bias_inner, w_attn_out, w_outer, temper):
    local = tokens.astype(jnp.float32)
    normed = (normalize(local) * norm_gain.astype(jnp.float32)).astype(jnp.bfloat16)
    query = jnp.dot(normed, w_query, preferred_element_type=jnp.float32).astype(jnp.bfloat16)
    keys = jnp.dot(normed, w_key, preferred_element_type=jnp.float32).astype(jnp.bfloat16)
    values = jnp.dot(normed, w_value, preferred_element_type=jnp.float32).astype(jnp.bfloat16)
    shape = (N_DP, PATCHES, HEADS, HEAD)
    query_norm = normalize(query.astype(jnp.float32).reshape(shape)).astype(jnp.bfloat16)
    key_norm = normalize(keys.astype(jnp.float32).reshape(shape)).astype(jnp.bfloat16)
    values4 = values.reshape(shape).astype(jnp.float32)
    scale = temper.astype(jnp.float32) / math.sqrt(HEAD)
    scores = jnp.einsum('bqhc,bkhc->bhqk', query_norm.astype(jnp.float32), key_norm.astype(jnp.float32))
    scores = scores * scale[None, :, None, None]
    probs = jax.nn.softmax(scores, axis=-1).astype(jnp.bfloat16)
    mixed = jnp.einsum('bhqk,bkhc->bqhc', probs.astype(jnp.float32), values4)
    mixed = mixed.astype(jnp.bfloat16).reshape(TOKENS, HD)
    inner = jnp.dot(normed, w_inner, preferred_element_type=jnp.float32) + bias_inner.astype(jnp.float32)
    activ = jax.nn.gelu(inner, approximate=False).astype(jnp.bfloat16)
    total = jnp.dot(mixed, w_attn_out, preferred_element_type=jnp.float32)
    total = total + jnp.dot(activ, w_outer, preferred_element_type=jnp.float32)
    return (local + total).astype(jnp.bfloat16)
```

```python
import functools
import math

import jax
import jax.numpy as jnp
from jax import lax
from jax.experimental import pallas as pl
from jax.experimental.pallas import tpu as pltpu
from jax.sharding import PartitionSpec as P

HEAD = 128
GROUP = 3
DIRECT_IN = ()
DIRECT_OUT = ()
MESH = pl.DeviceIdType.MESH
F32, BF16 = jnp.float32, jnp.bfloat16


def normalize(values):
    center = values - jnp.mean(values, axis=-1, keepdims=True)
    spread = jnp.mean(center * center, axis=-1, keepdims=True)
    return center * lax.rsqrt(spread + 1e-06)


def wait_bytes(ref, sem):
    pltpu.make_async_copy(ref, ref, sem).wait()


def block_kernel(
    n_dp, n_mp,
    tokens, gain, bias, temper, w_query, w_key, w_value, w_inner, w_attn, w_outer,
    out,
    tok, gain_v, bias_v, w_in, w_out, nsend, nrecv, stage, x, psend, precv, ag, acc,
    xsend, xrecv, dsend, drecv,
    in_sem, win_sem, wout_sem, a_send, a_recv, f_send, f_recv, p_send, p_recv, g_send, g_recv,
    x_send, x_recv, d_send, d_recv,
):
    rows = tok.shape[0]
    n_in, depth, wide = w_in.shape
    n_out = w_out.shape[0]
    per = psend.shape[2]
    i, j = lax.axis_index("dp"), lax.axis_index("mp")
    me = i * n_mp + j
    n_chip = n_mp // 2
    n_lane = n_dp * n_chip
    core, chip = lax.rem(j, 2), j // 2
    sibling = (i, j + 1 - 2 * core)
    lane = i * n_chip + chip
    square = n_dp == 4
    n_half = n_chip // 2
    spot = lax.rem(chip, n_half)
    halves = (chip // n_half, 1 - chip // n_half)

    inputs = [
        pltpu.make_async_copy(tokens, tok, in_sem.at[0]),
        pltpu.make_async_copy(gain, gain_v, in_sem.at[1]),
        pltpu.make_async_copy(bias, bias_v, in_sem.at[2]),
    ]
    for copy in inputs:
        copy.start()

    barrier = pltpu.get_barrier_semaphore()
    columns = [lax.rem(i + a, n_dp) for a in range(n_dp)]
    chips = [lax.rem(chip + b, n_chip) for b in range(n_chip)]
    for a in range(n_dp):
        for b in range(n_chip):
            if a or b:
                pl.semaphore_signal(
                    barrier, inc=1, device_id=(columns[a], 2 * chips[b] + core),
                    device_id_type=MESH,
                )
    pl.semaphore_signal(barrier, inc=1, device_id=sibling, device_id_type=MESH)

    for copy in inputs:
        copy.wait()
    for c, w in enumerate((w_query, w_key, w_value)):
        pltpu.make_async_copy(w, w_in.at[c], win_sem.at[0]).start()
    for c in range(3, n_in):
        pltpu.make_async_copy(
            w_inner.at[:, pl.ds((c - 3) * wide, wide)], w_in.at[c], win_sem.at[c // GROUP]
        ).start()
    pltpu.make_async_copy(w_attn, w_out.at[0], wout_sem.at[0]).start()
    for c in range(1, n_out):
        pltpu.make_async_copy(
            w_outer.at[pl.ds((c - 1) * wide, wide), :], w_out.at[c],
            wout_sem.at[(c - 1) // GROUP + 1],
        ).start()

    normed = (normalize(tok[...].astype(F32)) * gain_v[...]).astype(BF16)
    for p in range(n_dp):
        nsend[p] = normed[:, p * depth : (p + 1) * depth]
    nrecv[me] = nsend[i]
    pl.semaphore_wait(barrier, n_lane)

    def pass_on(source):
        pltpu.make_async_remote_copy(
            src_ref=nrecv.at[source], dst_ref=nrecv.at[source], send_sem=f_send, recv_sem=f_recv,
            device_id=sibling, device_id_type=MESH,
        ).start()

    for b in range(n_chip):
        for a in range(n_dp):
            if a or b:
                pltpu.make_async_remote_copy(
                    src_ref=nsend.at[columns[a]], dst_ref=nrecv.at[me],
                    send_sem=a_send, recv_sem=a_recv.at[b * n_dp + a],
                    device_id=(columns[a], 2 * chips[b] + core), device_id_type=MESH,
                ).start()
    pass_on(me)

    def forward(d, carry):
        wait_bytes(nrecv.at[0], a_recv.at[d])
        p = lax.rem(i + n_dp - lax.rem(d, n_dp), n_dp)
        q = lax.rem(chip + n_chip - d // n_dp, n_chip)
        pass_on(p * n_mp + 2 * q + core)
        return carry

    lax.fori_loop(1, n_lane, forward, 0)
    wait_bytes(nrecv.at[pl.ds(0, n_lane)], f_recv)
    for s in range(n_dp * n_mp):
        stage[s * rows : (s + 1) * rows, :] = nrecv[s].astype(F32)
    x[...] = stage[...].astype(BF16)

    def around(t):
        beside = i + 1 - 2 * lax.rem(i, 2)
        across = lax.rem(i + 2, n_dp)
        turn = lax.rem(t + core, 2)
        return beside + turn * (across - beside), across + turn * (beside - across)

    def send(source, target, send_sem, recv_sem, p):
        pltpu.make_async_remote_copy(
            src_ref=source, dst_ref=target, send_sem=send_sem, recv_sem=recv_sem,
            device_id=(p, j), device_id_type=MESH,
        ).start()

    def project(first, count):
        for r in range(count):
            c = first + r
            if c % GROUP == 0:
                wait_bytes(w_in.at[pl.ds(c, GROUP)], win_sem.at[c // GROUP])
        for r in range(count):
            c = first + r
            part = jnp.dot(x[...], w_in[c], preferred_element_type=F32).astype(BF16)
            psend[c] = part.reshape(n_dp, per, wide)
        for r in range(count):
            c = first + r
            if square and c not in DIRECT_IN:
                nearby, _ = around(c)
                send(psend.at[c, 3 - i], precv.at[c, 1], p_send, p_recv.at[c, 1], nearby)
                send(psend.at[c, nearby], precv.at[c, 0], p_send, p_recv.at[c, 0], nearby)
            else:
                precv[c, i] = psend[c, i]
                for d in range(1, n_dp):
                    p = lax.rem(i + d, n_dp)
                    send(psend.at[c, p], precv.at[c, i], p_send, p_recv.at[c, 0], p)

    def add_and_send(c):
        if not square or c in DIRECT_IN:
            return
        _, second = around(c)
        wait_bytes(precv.at[c, 1], p_recv.at[c, 1])
        precv[c, 3] = (psend[c, second].astype(F32) + precv[c, 1].astype(F32)).astype(BF16)
        send(precv.at[c, 3], precv.at[c, 2], p_send, p_recv.at[c, 2], second)

    def reduced(c):
        if square and c not in DIRECT_IN:
            wait_bytes(precv.at[c, 0], p_recv.at[c, 0])
            wait_bytes(precv.at[c, 2], p_recv.at[c, 2])
            total = psend[c, i].astype(F32) + precv[c, 0].astype(F32)
            return total + precv[c, 2].astype(F32)
        wait_bytes(precv.at[c, pl.ds(0, n_dp - 1)], p_recv.at[c, 0])
        total = precv[c, 0].astype(F32)
        for p in range(1, n_dp):
            total = total + precv[c, p].astype(F32)
        return total

    def hold(h, value):
        for half in range(2):
            ag[h, half, i] = value[half * (per // 2) : (half + 1) * (per // 2)]

    def block_of(h, half, p):
        return ag.at[h, :, p] if half is None else ag.at[h, halves[half], p]

    def lamp(h, half, step):
        return g_recv.at[h * 6 + 3 * (half or 0) + step]

    def share(h, half=None):
        own = block_of(h, half, i)
        if square and h not in DIRECT_OUT:
            first, second = around(h)
            send(own, own, g_send, lamp(h, half, 0), second)
            send(own, own, g_send, lamp(h, half, 1), first)
        else:
            for d in range(1, n_dp):
                send(own, own, g_send, lamp(h, half, 0), columns[d])

    def hand_over(h, half=None):
        if not square or h in DIRECT_OUT:
            return
        first, second = around(h)
        block = block_of(h, half, second)
        wait_bytes(block, lamp(h, half, 0))
        send(block, block, g_send, lamp(h, half, 2), first)

    def attend():
        query, key, value = (reduced(c).astype(BF16) for c in range(3))
        heads = range(wide // HEAD)
        cols = [slice(h * HEAD, (h + 1) * HEAD) for h in heads]
        tall = [t[:, cols[h]].astype(F32) for t in (query, key) for h in heads]
        tall = normalize(jnp.concatenate(tall, axis=0)).astype(BF16)
        pairs = [
            (tall[h * per : (h + 1) * per], tall[(len(heads) + h) * per : (len(heads) + h + 1) * per])
            for h in heads
        ]
        scores = jnp.concatenate([
            lax.dot_general(q, k, (((1,), (1,)), ((), ())), preferred_element_type=F32)
            * (temper[h] * (1.0 / math.sqrt(HEAD)))
            for h, (q, k) in zip(heads, pairs)
        ], axis=0)
        weight = jnp.exp(scores - jnp.max(scores, axis=-1, keepdims=True))
        probs = (weight / jnp.sum(weight, axis=-1, keepdims=True)).astype(BF16)
        mixed = [
            jnp.dot(
                probs[h * per : (h + 1) * per], value[:, cols[h]], preferred_element_type=F32
            ).astype(BF16)
            for h in heads
        ]
        hold(0, jnp.concatenate(mixed, axis=1))
        share(0)

    def activate(h, whole=True):
        at = (h - 1) * wide
        inner = reduced(h + 2) + bias_v[:, at : at + wide]
        activ = 0.5 * inner * (1.0 + lax.erf(inner * math.sqrt(0.5)))
        hold(h, activ.astype(BF16))
        if whole:
            share(h)

    def fetched(h, half=None):
        if half in (None, 1) and (h < 2 or (h - 1) % GROUP == 0):
            g = (h + GROUP - 1) // GROUP
            wait_bytes(w_out.at[pl.ds(0, min(h, 1) * (GROUP - 1) + 1)], wout_sem.at[g])
        block = block_of(h, half, 0)
        if square and h not in DIRECT_OUT:
            wait_bytes(block, lamp(h, half, 1))
            wait_bytes(block, lamp(h, half, 2))
        else:
            for d in range(1, n_dp):
                wait_bytes(block, lamp(h, half, 0))

    def project_out(hs, opened, half=None):
        for h in hs:
            fetched(h, half)
        total = None
        if opened:
            total = (acc[...] if half is None else acc[halves[half]]).reshape(-1, depth)
        for h in hs:
            left = (ag[h] if half is None else ag[h, halves[half]]).reshape(-1, wide)
            product = jnp.dot(left, w_out[h], preferred_element_type=F32)
            total = product if total is None else total + product
        if half is None:
            acc[...] = total.reshape(acc.shape)
        else:
            acc[halves[half]] = total.reshape(acc.shape[1:])

    def sorted_rows(half, p, q):
        tile = acc[halves[half], p, 2 * rows * q : 2 * rows * (q + 1), :]
        low, high = tile[:rows], tile[rows:]
        return jnp.where(core == 0, low, high), jnp.where(core == 0, high, low)

    def swap(half):
        for k in range(n_dp):
            p = columns[(k + 1) % n_dp]
            for q in range(n_half):
                xsend[half, p, q] = sorted_rows(half, p, q)[1].astype(BF16)
            pltpu.make_async_remote_copy(
                src_ref=xsend.at[half, p], dst_ref=xrecv.at[half, p],
                send_sem=x_send, recv_sem=x_recv.at[half, k],
                device_id=sibling, device_id_type=MESH,
            ).start()

    def deliver(half):
        for k in range(n_dp):
            p = columns[(k + 1) % n_dp]
            wait_bytes(xrecv.at[half, p], x_recv.at[half, k])
            for q in range(n_half):
                dsend[half, p, q] = (
                    sorted_rows(half, p, q)[0] + xrecv[half, p, q].astype(F32)
                ).astype(BF16)
            for b in list(range(1, n_half)) + [0]:
                if half or b or k < n_dp - 1:
                    q = lax.rem(spot + b, n_half)
                    pltpu.make_async_remote_copy(
                        src_ref=dsend.at[half, p, q], dst_ref=drecv.at[lane],
                        send_sem=d_send, recv_sem=d_recv,
                        device_id=(p, 2 * (halves[half] * n_half + q) + core),
                        device_id_type=MESH,
                    ).start()
        if not half:
            drecv[lane] = dsend[0, i, spot]

    project(0, 3)
    project(3, 3)
    for c in range(0, 3):
        add_and_send(c)
    project(6, 3)
    for c in range(3, 6):
        add_and_send(c)
    attend()
    for c in range(6, 9):
        add_and_send(c)
    for h in range(1, 4):
        activate(h)
    for h in range(0, 1):
        hand_over(h)
    for h in range(4, 7):
        activate(h)
    for h in range(1, 4):
        hand_over(h)
    project_out((0,), False)
    for h in range(4, 7):
        hand_over(h)
    project_out((1, 2), True)
    project_out((3,), True)
    project_out((4,), True)
    project_out((5,), True)
    project_out((6,), True)
    swap(1)
    deliver(1)
    swap(0)
    deliver(0)
    wait_bytes(drecv.at[pl.ds(0, n_lane - 1)], d_recv)
    for p in range(n_dp):
        total = drecv[p * n_chip].astype(F32)
        for q in range(1, n_chip):
            total = total + drecv[p * n_chip + q].astype(F32)
        cols = slice(p * depth, (p + 1) * depth)
        out[:, cols] = (tok[:, cols].astype(F32) + total).astype(BF16)

    wait_bytes(nrecv.at[pl.ds(0, n_lane - 1)], a_send)
    wait_bytes(nrecv.at[pl.ds(0, n_lane)], f_send)
    wait_bytes(precv.at[:, pl.ds(0, n_dp - 1)], p_send)
    wait_bytes(ag.at[:, :, pl.ds(0, n_dp - 1)], g_send)
    wait_bytes(xrecv, x_send)
    wait_bytes(drecv.at[pl.ds(0, n_lane - 1)], d_send)


def per_device(
    n_dp, n_mp,
    tokens, norm_gain, w_query, w_key, w_value, w_inner, bias_inner, w_attn_out, w_outer, temper
):
    rows, width = tokens.shape
    depth, wide = w_query.shape
    hidden = w_inner.shape[1]
    n_dev, per = n_dp * n_mp, n_mp * rows
    n_in, n_out = 3 + hidden // wide, 1 + hidden // wide
    vmem = pl.BlockSpec(memory_space=pltpu.VMEM)
    smem = pl.BlockSpec(memory_space=pltpu.SMEM)
    hbm = pl.BlockSpec(memory_space=pl.ANY)
    dma = pltpu.SemaphoreType.DMA
    return pl.pallas_call(
        functools.partial(block_kernel, n_dp, n_mp),
        out_shape=pltpu.VMEM((rows, width), BF16),
        in_specs=[hbm, hbm, hbm, smem] + [hbm] * 6,
        out_specs=vmem,
        scratch_shapes=[
            pltpu.VMEM((rows, width), BF16),
            pltpu.VMEM((1, width), F32),
            pltpu.VMEM((1, hidden), F32),
            pltpu.VMEM((n_in, depth, wide), BF16),
            pltpu.VMEM((n_out, wide, depth), BF16),
            pltpu.VMEM((n_dp, rows, depth), BF16),
            pltpu.VMEM((n_dev, rows, depth), BF16),
            pltpu.VMEM((n_dev * rows, depth), F32),
            pltpu.VMEM((n_dev * rows, depth), BF16),
            pltpu.VMEM((n_in, n_dp, per, wide), BF16),
            pltpu.VMEM((n_in, n_dp, per, wide), BF16),
            pltpu.VMEM((n_out, 2, n_dp, per // 2, wide), BF16),
            pltpu.VMEM((2, n_dp, per // 2, depth), F32),
            pltpu.VMEM((2, n_dp, n_mp // 4, rows, depth), BF16),
            pltpu.VMEM((2, n_dp, n_mp // 4, rows, depth), BF16),
            pltpu.VMEM((2, n_dp, n_mp // 4, rows, depth), BF16),
            pltpu.VMEM((n_dev // 2, rows, depth), BF16),
            dma((3,)), dma((n_in // GROUP,)), dma((n_in // GROUP,)), dma, dma((n_dev // 2,)),
            dma, dma, dma, dma((n_in, 3)), dma, dma((n_out * 6,)), dma, dma((2, n_dp)), dma, dma,
        ],
        compiler_params=pltpu.CompilerParams(
            collective_id=0, has_side_effects=True, vmem_limit_bytes=60 * 1024 * 1024
        ),
        name="encoder_block",
    )(
        tokens, norm_gain.reshape(1, -1), bias_inner.reshape(1, -1), temper,
        w_query, w_key, w_value, w_inner, w_attn_out, w_outer,
    )


def solution(mesh):
    return jax.shard_map(
        functools.partial(per_device, mesh.shape["dp"], mesh.shape["mp"]),
        mesh=mesh,
        in_specs=(
            P(("dp", "mp"), None),
            P(),
            P("dp", "mp"),
            P("dp", "mp"),
            P("dp", "mp"),
            P("dp", "mp"),
            P("mp"),
            P("mp", "dp"),
            P("mp", "dp"),
            P("mp"),
        ),
        out_specs=P(("dp", "mp"), None),
        check_vma=False,
    )
```

```python
import functools
import math

import jax
import jax.numpy as jnp
from jax import lax
from jax.experimental import pallas as pl
from jax.experimental.pallas import tpu as pltpu
from jax.sharding import PartitionSpec as P

HEAD = 128
GROUP = 3
MESH = pl.DeviceIdType.MESH
F32, BF16 = jnp.float32, jnp.bfloat16


def normalize(values):
    center = values - jnp.mean(values, axis=-1, keepdims=True)
    spread = jnp.mean(center * center, axis=-1, keepdims=True)
    return center * lax.rsqrt(spread + 1e-06)


def wait_bytes(ref, sem):
    pltpu.make_async_copy(ref, ref, sem).wait()


def block_kernel(
    n_dp, n_mp,
    tokens, gain, bias, temper, w_query, w_key, w_value, w_inner, w_attn, w_outer,
    out,
    tok, gain_v, bias_v, temper_v, w_in, w_out, nsend, nrecv, stage, x, psend, precv, ag, acc,
    xsend, xrecv, dsend, drecv,
    in_sem, win_sem, wout_sem, a_send, a_recv, f_send, f_recv, p_send, p_recv, g_send, g_recv,
    x_send, x_recv, d_send, d_recv,
):
    rows = tok.shape[0]
    n_in, depth, wide = w_in.shape
    n_out = w_out.shape[0]
    rows_half = psend.shape[2]
    per = 2 * rows_half
    n_group = n_in // GROUP
    i, j = lax.axis_index("dp"), lax.axis_index("mp")
    me = i * n_mp + j
    n_chip = n_mp // 2
    n_lane = n_dp * n_chip
    core, chip = lax.rem(j, 2), j // 2
    sibling = (i, j + 1 - 2 * core)
    lane = i * n_chip + chip
    square = n_dp == 4
    n_half = n_chip // 2
    spot = lax.rem(chip, n_half)
    halves = (chip // n_half, 1 - chip // n_half)

    inputs = [
        pltpu.make_async_copy(tokens, tok, in_sem.at[0]),
        pltpu.make_async_copy(gain, gain_v, in_sem.at[1]),
        pltpu.make_async_copy(bias, bias_v, in_sem.at[2]),
        pltpu.make_async_copy(temper, temper_v, in_sem.at[3]),
    ]
    for copy in inputs:
        copy.start()

    barrier = pltpu.get_barrier_semaphore()
    if square:
        beside, across = i + 1 - 2 * lax.rem(i, 2), lax.rem(i + 2, n_dp)
        columns = [i, beside, across, 3 - i]
    else:
        columns = [lax.rem(i + a, n_dp) for a in range(n_dp)]
    chips = [lax.rem(chip + b, n_chip) for b in range(n_chip)]
    for a in range(n_dp):
        for b in range(n_chip):
            if a or b:
                pl.semaphore_signal(
                    barrier, inc=1, device_id=(columns[a], 2 * chips[b] + core),
                    device_id_type=MESH,
                )
    pl.semaphore_signal(barrier, inc=1, device_id=sibling, device_id_type=MESH)

    for copy in inputs:
        copy.wait()
    normed = (normalize(tok[...].astype(F32)) * gain_v[...]).astype(BF16)
    for p in range(n_dp):
        nsend[p] = normed[:, p * depth : (p + 1) * depth]
    nrecv[me] = nsend[i]
    pl.semaphore_wait(barrier, n_lane)

    def pass_on(far, source):
        pltpu.make_async_remote_copy(
            src_ref=nrecv.at[source], dst_ref=nrecv.at[source],
            send_sem=f_send, recv_sem=f_recv.at[far],
            device_id=sibling, device_id_type=MESH,
        ).start()

    def outer_first(b):
        return b + (1 - halves[0]) * (n_half - 1 - 2 * b)

    for far in range(2):
        for b in range(n_half):
            b = b if far else n_half - 1 - b
            spot_to = outer_first(b) if far else lax.rem(spot + b, n_half)
            for a in reversed(range(n_dp)):
                if far or a or b:
                    pltpu.make_async_remote_copy(
                        src_ref=nsend.at[columns[a]], dst_ref=nrecv.at[me],
                        send_sem=a_send, recv_sem=a_recv.at[n_half + spot if far else b],
                        device_id=(columns[a], 2 * (halves[far] * n_half + spot_to) + core),
                        device_id_type=MESH,
                    ).start()
    pass_on(0, me)
    for c, w in enumerate((w_query, w_key, w_value)):
        pltpu.make_async_copy(w, w_in.at[c], win_sem.at[0]).start()
    for c in range(3, n_in):
        pltpu.make_async_copy(
            w_inner.at[:, pl.ds((c - 3) * wide, wide)], w_in.at[c], win_sem.at[c // GROUP]
        ).start()
    pltpu.make_async_copy(w_attn, w_out.at[0], wout_sem.at[0]).start()
    for c in range(1, n_out):
        pltpu.make_async_copy(
            w_outer.at[pl.ds((c - 1) * wide, wide), :], w_out.at[c],
            wout_sem.at[(c - 1) // GROUP + 1],
        ).start()

    def forward(far):
        for step in range(n_half):
            b = far * n_half + step
            spot_from = step if far else lax.rem(spot + n_half - step, n_half)
            source = 2 * (halves[far] * n_half + spot_from) + core
            first = 0 if b else 1
            wait_bytes(nrecv.at[pl.ds(0, n_dp - first)], a_recv.at[b])
            for a in range(first, n_dp):
                pass_on(far, columns[a] * n_mp + source)

    def gather(far):
        wait_bytes(nrecv.at[pl.ds(0, n_lane // 2)], f_recv.at[far])
        for p in range(n_dp):
            for k in range(n_chip):
                s = p * n_chip + k
                source = p * n_mp + halves[far] * n_chip + k
                stage[s * rows : (s + 1) * rows, :] = nrecv[source].astype(F32)
        x[far] = stage[...].astype(BF16)

    forward(0)
    gather(0)

    def around(t):
        turn = lax.rem(t + core, 2)
        return beside + turn * (across - beside), across + turn * (beside - across)

    def send(source, target, send_sem, recv_sem, p):
        pltpu.make_async_remote_copy(
            src_ref=source, dst_ref=target, send_sem=send_sem, recv_sem=recv_sem,
            device_id=(p, j), device_id_type=MESH,
        ).start()

    def project(far, g, early, fetch):
        if fetch:
            wait_bytes(w_in.at[pl.ds(g * GROUP, GROUP)], win_sem.at[g])
        def multiply(r):
            c = g * GROUP + r
            part = jnp.dot(x[far], w_in[c], preferred_element_type=F32).astype(BF16)
            psend[far * n_in + c] = part.reshape(n_dp, rows_half, wide)

        def scatter(r):
            t = far * n_in + g * GROUP + r
            lamp = p_recv.at[2 * (far * n_group + g)]
            if square:
                nearby, _ = around(t)
                send(psend.at[t, 3 - i], precv.at[t, 1], p_send, lamp, nearby)
                send(psend.at[t, nearby], precv.at[t, 0], p_send, lamp, nearby)
            else:
                precv[t, i] = psend[t, i]
                for d in range(1, n_dp):
                    send(psend.at[t, columns[d]], precv.at[t, i], p_send, lamp, columns[d])

        for r in range(GROUP):
            multiply(r)
            if r < early:
                scatter(r)
        for r in range(early, GROUP):
            scatter(r)

    def add_and_send(far, g):
        if not square:
            return
        u = far * n_group + g
        start = far * n_in + g * GROUP
        wait_bytes(precv.at[pl.ds(start, GROUP), pl.ds(0, 2)], p_recv.at[2 * u])
        seconds = [around(start + r)[1] for r in range(GROUP)]
        for r in range(GROUP):
            t = start + r
            precv[t, 3] = (psend[t, seconds[r]].astype(F32) + precv[t, 1].astype(F32)).astype(BF16)
        for r in range(GROUP):
            t = start + r
            send(precv.at[t, 3], precv.at[t, 2], p_send, p_recv.at[2 * u + 1], seconds[r])

    def arrived(far, g):
        u = far * n_group + g
        if square:
            wait_bytes(precv.at[pl.ds(far * n_in + g * GROUP, GROUP), 2], p_recv.at[2 * u + 1])
        else:
            start = far * n_in + g * GROUP
            wait_bytes(precv.at[pl.ds(start, GROUP), pl.ds(0, n_dp - 1)], p_recv.at[2 * u])

    def reduced(far, c):
        t = far * n_in + c
        if square:
            total = psend[t, i].astype(F32) + precv[t, 0].astype(F32)
            return total + precv[t, 2].astype(F32)
        total = precv[t, 0].astype(F32)
        for p in range(1, n_dp):
            total = total + precv[t, p].astype(F32)
        return total

    def members(g):
        return [0] if g == 0 else [(g - 1) * GROUP + 1 + r for r in range(GROUP)]

    def lamp_of(far, g, step):
        return g_recv.at[2 * (far * n_group + g) + min(step, 1)]

    def share(far, g):
        for h in members(g):
            own = ag.at[h, far, i]
            if square:
                first, second = around(h)
                send(own, own, g_send, lamp_of(far, g, 0), second)
                send(own, own, g_send, lamp_of(far, g, 1), first)
            else:
                for d in range(1, n_dp):
                    send(own, own, g_send, lamp_of(far, g, 0), columns[d])

    def hand_over(far, g):
        if not square:
            return
        hs = members(g)
        wait_bytes(ag.at[pl.ds(hs[0], len(hs)), far, 0], lamp_of(far, g, 0))
        for h in hs:
            first, second = around(h)
            block = ag.at[h, far, second]
            send(block, block, g_send, lamp_of(far, g, 2), first)

    def attend():
        for far in range(2):
            arrived(far, 0)
        query, key, value = (
            jnp.concatenate([reduced(0, c), reduced(1, c)], axis=0).astype(BF16) for c in range(3)
        )
        heads = range(wide // HEAD)
        cols = [slice(h * HEAD, (h + 1) * HEAD) for h in heads]
        tall = [t[:, cols[h]].astype(F32) for t in (query, key) for h in heads]
        tall = normalize(jnp.concatenate(tall, axis=0)).astype(BF16)
        pairs = [
            (tall[h * per : (h + 1) * per], tall[(len(heads) + h) * per : (len(heads) + h + 1) * per])
            for h in heads
        ]
        scores = jnp.concatenate([
            lax.dot_general(q, k, (((1,), (1,)), ((), ())), preferred_element_type=F32)
            * (temper_v[:, h : h + 1] * (1.0 / math.sqrt(HEAD)))
            for h, (q, k) in zip(heads, pairs)
        ], axis=0)
        weight = jnp.exp(scores - jnp.max(scores, axis=-1, keepdims=True))
        probs = (weight / jnp.sum(weight, axis=-1, keepdims=True)).astype(BF16)
        mixed = [
            jnp.dot(
                probs[h * per : (h + 1) * per], value[:, cols[h]], preferred_element_type=F32
            ).astype(BF16)
            for h in heads
        ]
        mixed = jnp.concatenate(mixed, axis=1)
        for far in range(2):
            ag[0, far, i] = mixed[far * rows_half : (far + 1) * rows_half]

    def activate(far, g):
        arrived(far, g)
        hs = members(g)
        values = []
        for h in hs:
            at = (h - 1) * wide
            inner = reduced(far, h + 2) + bias_v[:, at : at + wide]
            activ = 0.5 * inner * (1.0 + lax.erf(inner * math.sqrt(0.5)))
            values.append(activ.astype(BF16))
        for h, value in zip(hs, values):
            ag[h, far, i] = value

    def project_out(far, g, opened, fetch):
        hs = members(g)
        if fetch:
            wait_bytes(w_out.at[pl.ds(0, len(hs))], wout_sem.at[g])
        if square:
            both = ag.at[pl.ds(hs[0], len(hs)), far, pl.ds(0, 2)]
            wait_bytes(both, lamp_of(far, g, 1))
        else:
            wait_bytes(ag.at[pl.ds(hs[0], len(hs)), far, pl.ds(0, n_dp - 1)], lamp_of(far, g, 0))
        total = acc[far].reshape(-1, depth) if opened else None
        left = [ag[h, far].reshape(-1, wide) for h in hs]
        left = jnp.concatenate(left, axis=1) if len(hs) > 1 else left[0]
        right = w_out[hs[0] : hs[0] + len(hs)].reshape(-1, depth)
        product = jnp.dot(left, right, preferred_element_type=F32)
        total = product if total is None else total + product
        acc[far] = total.reshape(acc.shape[1:])

    def sorted_rows(half, p, q):
        tile = acc[half, p, 2 * rows * q : 2 * rows * (q + 1), :]
        low, high = tile[:rows], tile[rows:]
        return jnp.where(core == 0, low, high), jnp.where(core == 0, high, low)

    def swap(half):
        for k in range(n_dp):
            p = columns[n_dp - 1 - k]
            for q in range(n_half):
                xsend[half, p, q] = sorted_rows(half, p, q)[1].astype(BF16)
            pltpu.make_async_remote_copy(
                src_ref=xsend.at[half, p], dst_ref=xrecv.at[half, p],
                send_sem=x_send, recv_sem=x_recv.at[half],
                device_id=sibling, device_id_type=MESH,
            ).start()

    def deliver(half):
        wait_bytes(xrecv.at[half], x_recv.at[half])
        for k in range(n_dp):
            p = columns[n_dp - 1 - k]
            for q in range(n_half):
                dsend[half, p, q] = (
                    sorted_rows(half, p, q)[0] + xrecv[half, p, q].astype(F32)
                ).astype(BF16)
            for b in list(range(1, n_half)) + [0]:
                if half or b or k < n_dp - 1:
                    q = outer_first(b) if half else lax.rem(spot + b, n_half)
                    pltpu.make_async_remote_copy(
                        src_ref=dsend.at[half, p, q], dst_ref=drecv.at[lane],
                        send_sem=d_send, recv_sem=d_recv,
                        device_id=(p, 2 * (halves[half] * n_half + q) + core),
                        device_id_type=MESH,
                    ).start()
        if not half:
            drecv[lane] = dsend[0, i, spot]

    project(0, 0, 0, True)
    forward(1)
    project(0, 1, 0, True)
    gather(1)
    project(1, 1, 0, False)
    project(1, 2, 0, True)
    project(1, 0, 0, False)
    add_and_send(0, 0)
    add_and_send(0, 1)
    project(0, 2, 0, False)
    add_and_send(1, 1)
    add_and_send(1, 2)
    add_and_send(1, 0)
    add_and_send(0, 2)
    activate(0, 1)
    share(0, 1)
    activate(1, 1)
    share(1, 1)
    activate(1, 2)
    share(1, 2)
    attend()
    share(1, 0)
    share(0, 0)
    hand_over(0, 1)
    hand_over(1, 1)
    hand_over(1, 2)
    hand_over(1, 0)
    hand_over(0, 0)
    activate(0, 2)
    share(0, 2)
    project_out(0, 1, False, True)
    project_out(1, 1, False, False)
    project_out(1, 2, True, True)
    project_out(1, 0, True, True)
    swap(1)
    hand_over(0, 2)
    deliver(1)
    project_out(0, 0, True, False)
    project_out(0, 2, True, False)
    swap(0)
    deliver(0)
    wait_bytes(drecv.at[pl.ds(0, n_lane - 1)], d_recv)
    for p in range(n_dp):
        total = drecv[p * n_chip].astype(F32)
        for q in range(1, n_chip):
            total = total + drecv[p * n_chip + q].astype(F32)
        cols = slice(p * depth, (p + 1) * depth)
        out[:, cols] = (tok[:, cols].astype(F32) + total).astype(BF16)

    wait_bytes(nrecv.at[pl.ds(0, n_lane - 1)], a_send)
    wait_bytes(nrecv.at[pl.ds(0, n_lane)], f_send)
    wait_bytes(precv.at[:, pl.ds(0, n_dp - 1)], p_send)
    wait_bytes(ag.at[:, :, pl.ds(0, n_dp - 1)], g_send)
    wait_bytes(xrecv, x_send)
    wait_bytes(drecv.at[pl.ds(0, n_lane - 1)], d_send)


def per_device(
    n_dp, n_mp,
    tokens, norm_gain, w_query, w_key, w_value, w_inner, bias_inner, w_attn_out, w_outer, temper
):
    rows, width = tokens.shape
    depth, wide = w_query.shape
    hidden = w_inner.shape[1]
    n_dev, per = n_dp * n_mp, n_mp * rows
    n_in, n_out = 3 + hidden // wide, 1 + hidden // wide
    vmem = pl.BlockSpec(memory_space=pltpu.VMEM)
    hbm = pl.BlockSpec(memory_space=pl.ANY)
    dma = pltpu.SemaphoreType.DMA
    return pl.pallas_call(
        functools.partial(block_kernel, n_dp, n_mp),
        out_shape=pltpu.VMEM((rows, width), BF16),
        in_specs=[hbm] * 10,
        out_specs=vmem,
        scratch_shapes=[
            pltpu.VMEM((rows, width), BF16),
            pltpu.VMEM((1, width), F32),
            pltpu.VMEM((1, hidden), F32),
            pltpu.VMEM((1, wide // HEAD), F32),
            pltpu.VMEM((n_in, depth, wide), BF16),
            pltpu.VMEM((n_out, wide, depth), BF16),
            pltpu.VMEM((n_dp, rows, depth), BF16),
            pltpu.VMEM((n_dev, rows, depth), BF16),
            pltpu.VMEM((n_dev * rows // 2, depth), F32),
            pltpu.VMEM((2, n_dev * rows // 2, depth), BF16),
            pltpu.VMEM((2 * n_in, n_dp, per // 2, wide), BF16),
            pltpu.VMEM((2 * n_in, n_dp, per // 2, wide), BF16),
            pltpu.VMEM((n_out, 2, n_dp, per // 2, wide), BF16),
            pltpu.VMEM((2, n_dp, per // 2, depth), F32),
            pltpu.VMEM((2, n_dp, n_mp // 4, rows, depth), BF16),
            pltpu.VMEM((2, n_dp, n_mp // 4, rows, depth), BF16),
            pltpu.VMEM((2, n_dp, n_mp // 4, rows, depth), BF16),
            pltpu.VMEM((n_dev // 2, rows, depth), BF16),
            dma((4,)), dma((n_in // GROUP,)), dma((n_in // GROUP,)), dma, dma((n_mp // 2,)),
            dma, dma((2,)), dma, dma((4 * (n_in // GROUP),)), dma, dma((4 * (n_in // GROUP),)),
            dma, dma((2,)), dma, dma,
        ],
        compiler_params=pltpu.CompilerParams(
            collective_id=0, has_side_effects=True, vmem_limit_bytes=60 * 1024 * 1024
        ),
        name="encoder_block",
    )(
        tokens, norm_gain.reshape(1, -1), bias_inner.reshape(1, -1), temper.reshape(1, -1),
        w_query, w_key, w_value, w_inner, w_attn_out, w_outer,
    )


def solution(mesh):
    return jax.shard_map(
        functools.partial(per_device, mesh.shape["dp"], mesh.shape["mp"]),
        mesh=mesh,
        in_specs=(
            P(("dp", "mp"), None),
            P(),
            P("dp", "mp"),
            P("dp", "mp"),
            P("dp", "mp"),
            P("dp", "mp"),
            P("mp"),
            P("mp", "dp"),
            P("mp", "dp"),
            P("mp"),
        ),
        out_specs=P(("dp", "mp"), None),
        check_vma=False,
    )
```

```python
import functools
import math

import jax
import jax.numpy as jnp
from jax import lax
from jax.experimental import pallas as pl
from jax.experimental.pallas import tpu as pltpu
from jax.sharding import PartitionSpec as P

HEAD = 128
GROUP = 3
MESH = pl.DeviceIdType.MESH
F32, BF16 = jnp.float32, jnp.bfloat16


def normalize(values):
    center = values - jnp.mean(values, axis=-1, keepdims=True)
    spread = jnp.mean(center * center, axis=-1, keepdims=True)
    return center * lax.rsqrt(spread + 1e-06)


def wait_bytes(ref, sem):
    pltpu.make_async_copy(ref, ref, sem).wait()


def block_kernel(
    n_dp, n_mp,
    tokens, gain, bias, temper, w_query, w_key, w_value, w_inner, w_attn, w_outer,
    out,
    tok, gain_v, bias_v, temper_v, w_in, w_out, nsend, nrecv, stage, x, psend, precv, ag, acc,
    xsend, xrecv, dsend, drecv,
    in_sem, win_sem, wout_sem, a_send, a_recv, f_send, f_recv, p_send, p_recv, g_send, g_recv,
    x_send, x_recv, d_send, d_recv,
):
    rows = tok.shape[0]
    n_in, depth, wide = w_in.shape
    n_out = w_out.shape[0]
    rows_half = psend.shape[2]
    per = 2 * rows_half
    n_group = n_in // GROUP
    i, j = lax.axis_index("dp"), lax.axis_index("mp")
    me = i * n_mp + j
    n_chip = n_mp // 2
    n_lane = n_dp * n_chip
    core, chip = lax.rem(j, 2), j // 2
    sibling = (i, j + 1 - 2 * core)
    lane = i * n_chip + chip
    square = n_dp == 4
    n_half = n_chip // 2
    spot = lax.rem(chip, n_half)
    halves = (chip // n_half, 1 - chip // n_half)

    inputs = [
        pltpu.make_async_copy(tokens, tok, in_sem.at[0]),
        pltpu.make_async_copy(gain, gain_v, in_sem.at[1]),
        pltpu.make_async_copy(bias, bias_v, in_sem.at[2]),
        pltpu.make_async_copy(temper, temper_v, in_sem.at[3]),
    ]
    for copy in inputs:
        copy.start()

    barrier = pltpu.get_barrier_semaphore()
    if square:
        beside, across = i + 1 - 2 * lax.rem(i, 2), lax.rem(i + 2, n_dp)
        columns = [i, beside, across, 3 - i]
    else:
        columns = [lax.rem(i + a, n_dp) for a in range(n_dp)]
    chips = [lax.rem(chip + b, n_chip) for b in range(n_chip)]
    for a in range(n_dp):
        for b in range(n_chip):
            if a or b:
                pl.semaphore_signal(
                    barrier, inc=1, device_id=(columns[a], 2 * chips[b] + core),
                    device_id_type=MESH,
                )
    pl.semaphore_signal(barrier, inc=1, device_id=sibling, device_id_type=MESH)

    for copy in inputs:
        copy.wait()
    normed = (normalize(tok[...].astype(F32)) * gain_v[...]).astype(BF16)
    for p in range(n_dp):
        nsend[p] = normed[:, p * depth : (p + 1) * depth]
    nrecv[me] = nsend[i]
    pl.semaphore_wait(barrier, n_lane)

    def pass_on(far, source):
        pltpu.make_async_remote_copy(
            src_ref=nrecv.at[source], dst_ref=nrecv.at[source],
            send_sem=f_send, recv_sem=f_recv.at[far],
            device_id=sibling, device_id_type=MESH,
        ).start()

    def outer_first(b):
        return b + (1 - halves[0]) * (n_half - 1 - 2 * b)

    for far in range(2):
        for b in range(n_half):
            b = b if far else n_half - 1 - b
            spot_to = outer_first(b) if far else lax.rem(spot + b, n_half)
            for a in reversed(range(n_dp)):
                if far or a or b:
                    pltpu.make_async_remote_copy(
                        src_ref=nsend.at[columns[a]], dst_ref=nrecv.at[me],
                        send_sem=a_send, recv_sem=a_recv.at[n_half + spot if far else b],
                        device_id=(columns[a], 2 * (halves[far] * n_half + spot_to) + core),
                        device_id_type=MESH,
                    ).start()
    pass_on(0, me)
    for c, w in enumerate((w_query, w_key, w_value)):
        pltpu.make_async_copy(w, w_in.at[c], win_sem.at[0]).start()
    for c in range(3, n_in):
        pltpu.make_async_copy(
            w_inner.at[:, pl.ds((c - 3) * wide, wide)], w_in.at[c], win_sem.at[c // GROUP]
        ).start()
    pltpu.make_async_copy(w_attn, w_out.at[0], wout_sem.at[0]).start()
    for c in range(1, n_out):
        pltpu.make_async_copy(
            w_outer.at[pl.ds((c - 1) * wide, wide), :], w_out.at[c],
            wout_sem.at[(c - 1) // GROUP + 1],
        ).start()

    def forward(far):
        for step in range(n_half):
            b = far * n_half + step
            spot_from = step if far else lax.rem(spot + n_half - step, n_half)
            source = 2 * (halves[far] * n_half + spot_from) + core
            first = 0 if b else 1
            wait_bytes(nrecv.at[pl.ds(0, n_dp - first)], a_recv.at[b])
            for a in range(first, n_dp):
                pass_on(far, columns[a] * n_mp + source)

    def gather(far):
        wait_bytes(nrecv.at[pl.ds(0, n_lane // 2)], f_recv.at[far])
        for p in range(n_dp):
            for k in range(n_chip):
                s = p * n_chip + k
                source = p * n_mp + halves[far] * n_chip + k
                stage[s * rows : (s + 1) * rows, :] = nrecv[source].astype(F32)
        x[far] = stage[...].astype(BF16)

    forward(0)
    gather(0)

    def around(t):
        turn = lax.rem(t + core, 2)
        return beside + turn * (across - beside), across + turn * (beside - across)

    def send(source, target, send_sem, recv_sem, p):
        pltpu.make_async_remote_copy(
            src_ref=source, dst_ref=target, send_sem=send_sem, recv_sem=recv_sem,
            device_id=(p, j), device_id_type=MESH,
        ).start()

    def project(far, g, early, fetch):
        if fetch:
            wait_bytes(w_in.at[pl.ds(g * GROUP, GROUP)], win_sem.at[g])
        def multiply(r):
            c = g * GROUP + r
            part = jnp.dot(x[far], w_in[c], preferred_element_type=F32).astype(BF16)
            psend[far * n_in + c] = part.reshape(n_dp, rows_half, wide)

        def scatter(r):
            t = far * n_in + g * GROUP + r
            lamp = p_recv.at[2 * (far * n_group + g)]
            if square:
                nearby, _ = around(t)
                send(psend.at[t, 3 - i], precv.at[t, 1], p_send, lamp, nearby)
                send(psend.at[t, nearby], precv.at[t, 0], p_send, lamp, nearby)
            else:
                precv[t, i] = psend[t, i]
                for d in range(1, n_dp):
                    send(psend.at[t, columns[d]], precv.at[t, i], p_send, lamp, columns[d])

        for r in range(GROUP):
            multiply(r)
            if r < early:
                scatter(r)
        for r in range(early, GROUP):
            scatter(r)

    def add_and_send(far, g):
        if not square:
            return
        u = far * n_group + g
        start = far * n_in + g * GROUP
        wait_bytes(precv.at[pl.ds(start, GROUP), pl.ds(0, 2)], p_recv.at[2 * u])
        seconds = [around(start + r)[1] for r in range(GROUP)]
        for r in range(GROUP):
            t = start + r
            precv[t, 3] = (psend[t, seconds[r]].astype(F32) + precv[t, 1].astype(F32)).astype(BF16)
        for r in range(GROUP):
            t = start + r
            send(precv.at[t, 3], precv.at[t, 2], p_send, p_recv.at[2 * u + 1], seconds[r])

    def arrived(far, g):
        u = far * n_group + g
        if square:
            wait_bytes(precv.at[pl.ds(far * n_in + g * GROUP, GROUP), 2], p_recv.at[2 * u + 1])
        else:
            start = far * n_in + g * GROUP
            wait_bytes(precv.at[pl.ds(start, GROUP), pl.ds(0, n_dp - 1)], p_recv.at[2 * u])

    def reduced(far, c):
        t = far * n_in + c
        if square:
            total = psend[t, i].astype(F32) + precv[t, 0].astype(F32)
            return total + precv[t, 2].astype(F32)
        total = precv[t, 0].astype(F32)
        for p in range(1, n_dp):
            total = total + precv[t, p].astype(F32)
        return total

    def members(g):
        return [0] if g == 0 else [(g - 1) * GROUP + 1 + r for r in range(GROUP)]

    def lamp_of(far, g, step):
        return g_recv.at[2 * (far * n_group + g) + min(step, 1)]

    def share(far, g):
        for h in members(g):
            own = ag.at[h, far, i]
            if square:
                first, second = around(h)
                send(own, own, g_send, lamp_of(far, g, 0), second)
                send(own, own, g_send, lamp_of(far, g, 1), first)
            else:
                for d in range(1, n_dp):
                    send(own, own, g_send, lamp_of(far, g, 1), columns[d])

    def hand_over(far, g):
        if not square:
            return
        hs = members(g)
        wait_bytes(ag.at[pl.ds(hs[0], len(hs)), far, 0], lamp_of(far, g, 0))
        for h in hs:
            first, second = around(h)
            block = ag.at[h, far, second]
            send(block, block, g_send, lamp_of(far, g, 2), first)

    def attend():
        for far in range(2):
            arrived(far, 0)
        query, key, value = (
            jnp.concatenate([reduced(0, c), reduced(1, c)], axis=0).astype(BF16) for c in range(3)
        )
        heads = range(wide // HEAD)
        cols = [slice(h * HEAD, (h + 1) * HEAD) for h in heads]
        tall = [t[:, cols[h]].astype(F32) for t in (query, key) for h in heads]
        tall = normalize(jnp.concatenate(tall, axis=0)).astype(BF16)
        pairs = [
            (tall[h * per : (h + 1) * per], tall[(len(heads) + h) * per : (len(heads) + h + 1) * per])
            for h in heads
        ]
        scores = jnp.concatenate([
            lax.dot_general(q, k, (((1,), (1,)), ((), ())), preferred_element_type=F32)
            * (temper_v[:, h : h + 1] * (1.0 / math.sqrt(HEAD)))
            for h, (q, k) in zip(heads, pairs)
        ], axis=0)
        weight = jnp.exp(scores - jnp.max(scores, axis=-1, keepdims=True))
        probs = (weight / jnp.sum(weight, axis=-1, keepdims=True)).astype(BF16)
        mixed = [
            jnp.dot(
                probs[h * per : (h + 1) * per], value[:, cols[h]], preferred_element_type=F32
            ).astype(BF16)
            for h in heads
        ]
        mixed = jnp.concatenate(mixed, axis=1)
        for far in range(2):
            ag[0, far, i] = mixed[far * rows_half : (far + 1) * rows_half]

    def activate(far, g):
        arrived(far, g)
        hs = members(g)
        values = []
        for h in hs:
            at = (h - 1) * wide
            inner = reduced(far, h + 2) + bias_v[:, at : at + wide]
            activ = 0.5 * inner * (1.0 + lax.erf(inner * math.sqrt(0.5)))
            values.append(activ.astype(BF16))
        for h, value in zip(hs, values):
            ag[h, far, i] = value

    def project_out(far, g, opened, fetch):
        hs = members(g)
        if fetch:
            wait_bytes(w_out.at[pl.ds(0, len(hs))], wout_sem.at[g])
        others = 2 if square else n_dp - 1
        wait_bytes(ag.at[pl.ds(hs[0], len(hs)), far, pl.ds(0, others)], lamp_of(far, g, 1))
        total = acc[far].reshape(-1, depth) if opened else None
        left = [ag[h, far].reshape(-1, wide) for h in hs]
        left = jnp.concatenate(left, axis=1) if len(hs) > 1 else left[0]
        right = w_out[hs[0] : hs[0] + len(hs)].reshape(-1, depth)
        product = jnp.dot(left, right, preferred_element_type=F32)
        total = product if total is None else total + product
        acc[far] = total.reshape(acc.shape[1:])

    def sorted_rows(half, p, q):
        tile = acc[half, p, 2 * rows * q : 2 * rows * (q + 1), :]
        low, high = tile[:rows], tile[rows:]
        return jnp.where(core == 0, low, high), jnp.where(core == 0, high, low)

    def swap(half):
        for k in range(n_dp):
            p = columns[n_dp - 1 - k]
            for q in range(n_half):
                xsend[half, p, q] = sorted_rows(half, p, q)[1].astype(BF16)
            pltpu.make_async_remote_copy(
                src_ref=xsend.at[half, p], dst_ref=xrecv.at[half, p],
                send_sem=x_send, recv_sem=x_recv.at[half],
                device_id=sibling, device_id_type=MESH,
            ).start()

    def deliver(half):
        wait_bytes(xrecv.at[half], x_recv.at[half])
        for k in range(n_dp):
            p = columns[n_dp - 1 - k]
            for q in range(n_half):
                dsend[half, p, q] = (
                    sorted_rows(half, p, q)[0] + xrecv[half, p, q].astype(F32)
                ).astype(BF16)
            for b in list(range(1, n_half)) + [0]:
                if half or b or k < n_dp - 1:
                    q = outer_first(b) if half else lax.rem(spot + b, n_half)
                    pltpu.make_async_remote_copy(
                        src_ref=dsend.at[half, p, q], dst_ref=drecv.at[lane],
                        send_sem=d_send, recv_sem=d_recv,
                        device_id=(p, 2 * (halves[half] * n_half + q) + core),
                        device_id_type=MESH,
                    ).start()
        if not half:
            drecv[lane] = dsend[0, i, spot]

    project(0, 0, 0, True)
    forward(1)
    project(0, 1, 0, True)
    gather(1)
    project(1, 1, 0, False)
    project(1, 2, 0, True)
    project(1, 0, 0, False)
    add_and_send(0, 0)
    add_and_send(0, 1)
    add_and_send(1, 1)
    project(0, 2, 0, False)
    add_and_send(1, 2)
    add_and_send(1, 0)
    activate(0, 1)
    share(0, 1)
    add_and_send(0, 2)
    activate(1, 1)
    share(1, 1)
    activate(1, 2)
    share(1, 2)
    attend()
    share(1, 0)
    share(0, 0)
    hand_over(0, 1)
    hand_over(1, 1)
    hand_over(1, 2)
    hand_over(1, 0)
    hand_over(0, 0)
    activate(0, 2)
    share(0, 2)
    project_out(0, 1, False, True)
    project_out(1, 1, False, False)
    project_out(1, 2, True, True)
    project_out(1, 0, True, True)
    swap(1)
    hand_over(0, 2)
    deliver(1)
    project_out(0, 0, True, False)
    project_out(0, 2, True, False)
    swap(0)
    deliver(0)
    wait_bytes(drecv.at[pl.ds(0, n_lane - 1)], d_recv)
    for p in range(n_dp):
        total = drecv[p * n_chip].astype(F32)
        for q in range(1, n_chip):
            total = total + drecv[p * n_chip + q].astype(F32)
        cols = slice(p * depth, (p + 1) * depth)
        out[:, cols] = (tok[:, cols].astype(F32) + total).astype(BF16)

    wait_bytes(nrecv.at[pl.ds(0, n_lane - 1)], a_send)
    wait_bytes(nrecv.at[pl.ds(0, n_lane)], f_send)
    wait_bytes(precv.at[:, pl.ds(0, n_dp - 1)], p_send)
    wait_bytes(ag.at[:, :, pl.ds(0, n_dp - 1)], g_send)
    wait_bytes(xrecv, x_send)
    wait_bytes(drecv.at[pl.ds(0, n_lane - 1)], d_send)


def per_device(
    n_dp, n_mp,
    tokens, norm_gain, w_query, w_key, w_value, w_inner, bias_inner, w_attn_out, w_outer, temper
):
    rows, width = tokens.shape
    depth, wide = w_query.shape
    hidden = w_inner.shape[1]
    n_dev, per = n_dp * n_mp, n_mp * rows
    n_in, n_out = 3 + hidden // wide, 1 + hidden // wide
    vmem = pl.BlockSpec(memory_space=pltpu.VMEM)
    hbm = pl.BlockSpec(memory_space=pl.ANY)
    dma = pltpu.SemaphoreType.DMA
    return pl.pallas_call(
        functools.partial(block_kernel, n_dp, n_mp),
        out_shape=pltpu.VMEM((rows, width), BF16),
        in_specs=[hbm] * 10,
        out_specs=vmem,
        scratch_shapes=[
            pltpu.VMEM((rows, width), BF16),
            pltpu.VMEM((1, width), F32),
            pltpu.VMEM((1, hidden), F32),
            pltpu.VMEM((1, wide // HEAD), F32),
            pltpu.VMEM((n_in, depth, wide), BF16),
            pltpu.VMEM((n_out, wide, depth), BF16),
            pltpu.VMEM((n_dp, rows, depth), BF16),
            pltpu.VMEM((n_dev, rows, depth), BF16),
            pltpu.VMEM((n_dev * rows // 2, depth), F32),
            pltpu.VMEM((2, n_dev * rows // 2, depth), BF16),
            pltpu.VMEM((2 * n_in, n_dp, per // 2, wide), BF16),
            pltpu.VMEM((2 * n_in, n_dp, per // 2, wide), BF16),
            pltpu.VMEM((n_out, 2, n_dp, per // 2, wide), BF16),
            pltpu.VMEM((2, n_dp, per // 2, depth), F32),
            pltpu.VMEM((2, n_dp, n_mp // 4, rows, depth), BF16),
            pltpu.VMEM((2, n_dp, n_mp // 4, rows, depth), BF16),
            pltpu.VMEM((2, n_dp, n_mp // 4, rows, depth), BF16),
            pltpu.VMEM((n_dev // 2, rows, depth), BF16),
            dma((4,)), dma((n_in // GROUP,)), dma((n_in // GROUP,)), dma, dma((n_mp // 2,)),
            dma, dma((2,)), dma, dma((4 * (n_in // GROUP),)), dma, dma((4 * (n_in // GROUP),)),
            dma, dma((2,)), dma, dma,
        ],
        compiler_params=pltpu.CompilerParams(
            collective_id=0, has_side_effects=True, vmem_limit_bytes=60 * 1024 * 1024
        ),
        name="encoder_block",
    )(
        tokens, norm_gain.reshape(1, -1), bias_inner.reshape(1, -1), temper.reshape(1, -1),
        w_query, w_key, w_value, w_inner, w_attn_out, w_outer,
    )


def solution(mesh):
    return jax.shard_map(
        functools.partial(per_device, mesh.shape["dp"], mesh.shape["mp"]),
        mesh=mesh,
        in_specs=(
            P(("dp", "mp"), None),
            P(),
            P("dp", "mp"),
            P("dp", "mp"),
            P("dp", "mp"),
            P("dp", "mp"),
            P("mp"),
            P("mp", "dp"),
            P("mp", "dp"),
            P("mp"),
        ),
        out_specs=P(("dp", "mp"), None),
        check_vma=False,
    )
```
